768 devices in a mesh: rep: 96 (over x, z, core), shard: 8 (over y).
Axes of the slice: x: 4, y: 8, z: 12, core: 2. Of those that a mesh axis runs over, the one named last changes fastest.
Arguments:
- inputs: bfloat16 [36864, 2048], P('rep', 'shard'), may hold values from -6 to 6
- cotangent: bfloat16 [36864, 6144], P('rep'), may hold values from -0.109375 to 0.109375
- momentum: float32 [6144, 2048], P('rep', 'shard'), may hold values from -54 to 54
- right_prev: float32 [2048, 64], P('shard'), may hold values from -0.125 to 0.125
Outputs:
- new_momentum: float32 [6144, 2048], P('rep', 'shard')
- right_factor: float32 [2048, 64], P('shard')
- update: bfloat16 [6144, 2048], P('rep', 'shard')
The draws below stay inside these ranges and needn't reach their ends.
All inputs are finite; a program needn't handle non-finite values.
Results may differ from the reference program's by a relative error of at most 0.001.
Values sent between devices are 32-bit elements; how exact they have to be, the bound alone decides.
No kernel may reach another device: no remote copies, remote signals or barrier semaphores. Data moves between devices by JAX's collectives and lax.ppermute only.
A program may use at most 64 MiB of HBM per device.

```python
import math
import jax
import jax.numpy as jnp
from jax import lax

R = 64
OUT = 6144
IN = 2048
TOKENS = 36864


def draw_momentum(key, part):
    first_key, second_key = jax.random.split(key, 2)
    position = jnp.arange(OUT, dtype=jnp.float32) / max(OUT - 1, 1)
    ramp_scale = 1.0 + 2.0 * position
    row_scale = jnp.exp(jax.random.uniform(second_key, (OUT, 1), jnp.float32, math.log(0.3), math.log(3.0)))
    base_draw = jax.random.normal(first_key, (OUT, IN), jnp.float32)
    base_draw = jnp.clip(base_draw, -6.0, 6.0)
    return base_draw * row_scale * ramp_scale[:, None]


def raised(entries, rng, source, target, parts, factor):
    owner, partner = [(jnp.arange(entries.shape[dim]) // (entries.shape[dim] // parts)).reshape([-1 if axis == dim else 1 for axis in range(entries.ndim)]) for dim in (source, target)]
    chosen = jax.random.permutation(rng, parts)[partner]
    strong = (owner == chosen) | (owner == (partner + parts // 2) % parts)
    return jnp.where(strong, factor * entries, entries)


def block_levels(own_key, dims, cuts, least, top_value):
    def one(axis_at, blocks):
        heights = jax.random.uniform(jax.random.fold_in(jax.random.fold_in(own_key, 6), axis_at), (blocks,), jnp.float32, least / len(cuts), top_value / len(cuts))
        return jnp.repeat(jnp.exp(heights), dims[axis_at] // blocks).reshape((-1,) + (1,) * (len(dims) - axis_at - 1))

    loudness = one(*cuts[0])
    for cut in cuts[1:]:
        loudness = loudness * one(*cut)
    return loudness


def noise(rng, dims, scale, reach, pieces=(), kind=jnp.bfloat16):
    values = jax.random.normal(rng, dims, jnp.float32) * scale
    if len(pieces) > 0:
        values = block_levels(rng, dims, pieces, -0.22, 0.18) * values
    return jnp.clip(values, min=-reach, max=reach).astype(kind)


def bell_draw_with(stream_key, extent, deviation, reach, pieces, heavy, kind=jnp.bfloat16):
    drawn = deviation * jax.random.normal(stream_key, extent, jnp.float32)
    if pieces:
        drawn = drawn * block_levels(stream_key, extent, pieces, -0.22, 0.18)
    return jnp.clip(raised(drawn, jax.random.fold_in(stream_key, 3), *heavy), -reach, reach).astype(kind)


def setup_inputs(seed: int = 0) -> dict:
    streams_of = jax.random.split(jax.random.key(seed), 5)
    inputs = noise(streams_of[0], (TOKENS, IN), 1.0, 6.0, ((0, 96), (1, 8)))
    cotangent = bell_draw_with(streams_of[1], (TOKENS, OUT), TOKENS ** -0.5, 0.109375, ((0, 96),), (0, 1, 96, 4.75))
    momentum = draw_momentum(jax.random.fold_in(streams_of[4], 71), 0)
    right_prev = noise(streams_of[3], (IN, R), IN ** -0.5, 0.125, ((0, 8),), jnp.float32)
    return {"inputs": inputs, "cotangent": cotangent, "momentum": momentum, "right_prev": right_prev}


def reference(inputs, cotangent, momentum, right_prev):
    high = lax.Precision.HIGHEST
    gradient = lax.dot_general(cotangent.astype(jnp.float32), inputs.astype(jnp.float32), (((0,), (0,)), ((), ())), precision=high, preferred_element_type=jnp.float32)
    blended = momentum + gradient
    left_raw = jnp.dot(blended, right_prev, precision=high)
    gram_sum = jnp.dot(left_raw.T, left_raw, precision=high)
    lower_factor = jnp.linalg.cholesky(gram_sum)
    ortho = lax.linalg.triangular_solve(lower_factor, left_raw.T, left_side=True, lower=True).T
    right_raw = jnp.dot(blended.T, ortho, precision=high)
    new_momentum = blended - 0.05 * jnp.dot(ortho, right_raw.T, precision=high)
    column_sq = lax.optimization_barrier(jnp.sum(right_raw * right_raw, axis=0))
    right_factor = right_raw / jnp.sqrt(column_sq + 1e-06)
    scale_factor = (OUT * IN / R) ** 0.5
    update = (scale_factor * jnp.dot(ortho, right_factor.T, precision=high)).astype(jnp.bfloat16)
    return (new_momentum, right_factor, update)
```

```python
import jax
import jax.numpy as jnp
from jax import lax
from jax.sharding import Mesh
from jax.sharding import PartitionSpec as P

X, ZA, ZB, CORE, SHARD = "rep_x", "rep_za", "rep_zb", "rep_core", "shard"
REP = (X, ZA, ZB, CORE)
HIGH = lax.Precision.HIGHEST


def exchanged(pieces, axis):
    return lax.all_to_all(pieces, axis, 0, 0, tiled=True)


def scattered_sum(pieces, axis):
    return jnp.sum(exchanged(pieces, axis), axis=0)


def from_everyone(value, axis):
    count = lax.axis_size(axis)
    return exchanged(jnp.broadcast_to(value[None], (count, *value.shape)), axis)


def gradient_rows(inputs, cotangent):
    nx, na, nb = (lax.axis_size(a) for a in (X, ZA, ZB))
    partial = lax.dot_general(
        cotangent, inputs, (((0,), (0,)), ((), ())), preferred_element_type=jnp.float32
    )
    rows, cols = partial.shape[0] // (nx * na * nb * 2), partial.shape[1]
    halves = partial.reshape(nx * na * nb, 2, rows, cols)
    core = lax.axis_index(CORE)
    mine = lax.dynamic_index_in_dim(halves, core, 1, keepdims=False)
    other = lax.dynamic_index_in_dim(halves, 1 - core, 1, keepdims=False)
    chip = mine + lax.ppermute(other, CORE, ((0, 1), (1, 0)))
    over_x = scattered_sum(chip.reshape(nx, na * nb * rows, cols), X)
    by_zb = over_x.reshape(na, nb, rows, cols).transpose(1, 0, 2, 3)
    over_zb = scattered_sum(by_zb.reshape(nb, na * rows, cols), ZB)
    return scattered_sum(over_zb.reshape(na, rows, cols), ZA)


def rep_total(value):
    members = lax.axis_size((X, CORE))
    piece = scattered_sum(value.reshape(members, value.shape[0] // members, value.shape[1]), (X, CORE))
    piece = jnp.sum(from_everyone(piece, (ZA, ZB)), axis=0)
    return from_everyone(piece, (X, CORE)).reshape(value.shape)


def body(inputs, cotangent, momentum, right_prev):
    out_total = cotangent.shape[1]
    in_total = momentum.shape[1] * lax.axis_size(SHARD)
    rank = right_prev.shape[1]
    cols = momentum.shape[1]
    blended = momentum + gradient_rows(inputs, cotangent)
    left_part = jnp.dot(blended, right_prev, precision=HIGH)
    half = left_part.shape[0] // 2
    packed = jnp.concatenate([left_part[:half], left_part[half:]], axis=1)
    packed = jnp.sum(from_everyone(packed, SHARD), axis=0)
    left_raw = jnp.concatenate([packed[:, :rank], packed[:, rank:]], axis=0)
    both = jnp.concatenate([blended, left_raw, jnp.zeros_like(left_raw)], axis=1)
    total = rep_total(lax.dot_general(left_raw, both, (((0,), (0,)), ((), ())), precision=HIGH))
    projected, gram_sum = total[:, :cols], total[:, cols : cols + rank]
    lower_factor = jnp.linalg.cholesky(gram_sum)
    inverse = lax.linalg.triangular_solve(
        lower_factor, jnp.eye(rank, dtype=jnp.float32), left_side=True, lower=True
    )
    ortho = lax.dot_general(left_raw, inverse, (((1,), (1,)), ((), ())), precision=HIGH)
    right_rows = jnp.dot(inverse, projected, precision=HIGH)
    column_sq = jnp.sum(from_everyone(jnp.sum(right_rows * right_rows, axis=1), SHARD), axis=0)
    new_momentum = blended - 0.05 * jnp.dot(ortho, right_rows, precision=HIGH)
    factor_rows = right_rows / jnp.sqrt(column_sq + 1e-06)[:, None]
    scale_factor = (out_total * in_total / rank) ** 0.5
    update = (scale_factor * jnp.dot(ortho, factor_rows, precision=HIGH)).astype(jnp.bfloat16)
    return (new_momentum, factor_rows.T, update)


def solution(mesh):
    finer = Mesh(mesh.devices.reshape(4, 4, 3, 2, mesh.shape["shard"]), (*REP, SHARD))
    in_specs = (P(REP, SHARD), P(REP, None), P(REP, SHARD), P(SHARD, None))
    out_specs = (P(REP, SHARD), P(SHARD, None), P(REP, SHARD))
    return jax.shard_map(body, mesh=finer, in_specs=in_specs, out_specs=out_specs, check_vma=False)
```

```python
import functools

import jax
import jax.numpy as jnp
from jax import lax
from jax.experimental import pallas as pl
from jax.experimental.pallas import tpu as pltpu
from jax.sharding import Mesh
from jax.sharding import PartitionSpec as P

X, Z, CORE, SHARD = "rep_x", "rep_z", "rep_core", "shard"
REP = (X, Z, CORE)
CLASSES = 3
HIGH = lax.Precision.HIGHEST


def exchanged(pieces, axis, groups=None):
    return lax.all_to_all(pieces, axis, 0, 0, tiled=True, axis_index_groups=groups)


def from_everyone(value, axis):
    count = lax.axis_size(axis)
    return exchanged(jnp.broadcast_to(value[None], (count, *value.shape)), axis)


def sent(value, axis, distance):
    size = lax.axis_size(axis)
    return lax.ppermute(value, axis, [(i, (i + distance) % size) for i in range(size)])


def gated(value, *earlier):
    return lax.optimization_barrier((value, *earlier))[0]


def gradient_rows(inputs, cotangent):
    nx, nz = lax.axis_size(X), lax.axis_size(Z)
    na, nb = nz // CLASSES, CLASSES
    cols = inputs.shape[1]
    rows = cotangent.shape[1] // (nx * nz * 2)
    x, z, core = lax.axis_index(X), lax.axis_index(Z), lax.axis_index(CORE)
    half = na // 2

    partial = lax.dot_general(
        cotangent, inputs, (((0,), (0,)), ((), ())), preferred_element_type=jnp.float32
    ).reshape(nx, na, nb, 2, rows, cols)

    def piece(ahead, which):
        at_x = lax.dynamic_index_in_dim(partial, (x + ahead) % nx, 0, keepdims=False)
        return lax.dynamic_index_in_dim(at_x, which, 2, keepdims=False)

    far = sent(piece(2, 1 - core), CORE, 1)
    near = jnp.stack([piece(ahead, 1 - core) for ahead in (1, 3, 0)])
    near = sent(near, CORE, 1)
    mine = piece(2, core)
    far_up, far_down = mine[:half] + far[:half], mine[half:] + far[half:]
    relay_up = sent(far_up, X, 1)
    relay_down = sent(far_down, X, -1)
    near = gated(near, far_up, far_down)
    before, after = piece(1, core), piece(3, core)
    before_low, before_high = before[:half] + near[0, :half], before[half:] + near[0, half:]
    after_low, after_high = after[:half] + near[1, :half], after[half:] + near[1, half:]
    high_below = sent(before_high, X, 1)
    low_above = sent(after_low, X, -1)
    relay_up = gated(relay_up, before_low, before_high, after_low)
    low_below = sent(before_low + relay_up, X, 1)
    relay_down = gated(relay_down, after_high, before_high, after_low)
    high_above = sent(after_high + relay_down, X, -1)
    own = lax.optimization_barrier(piece(0, core) + near[2])
    low = own[:half] + low_below + low_above
    high = own[half:] + high_below + high_above
    over_x = jnp.concatenate([low, high], axis=0)

    kind = z % nb

    def of_class(ahead):
        return lax.dynamic_index_in_dim(over_x, (kind + ahead) % nb, 1, keepdims=False)

    up = sent(of_class(1), Z, 1)
    down = sent(of_class(nb - 1), Z, -1)
    over_near_z = of_class(0) + up + down
    groups = [[a * nb + b for a in range(na)] for b in range(nb)]
    return exchanged(over_near_z, Z, groups)


def rep_total(value):
    members = lax.axis_size((X, CORE))
    piece = value.reshape(members, value.shape[0] // members, value.shape[1])
    piece = jnp.sum(exchanged(piece, (X, CORE)), axis=0)
    piece = jnp.sum(from_everyone(piece, Z), axis=0)
    return from_everyone(piece, (X, CORE)).reshape(value.shape)


def eliminate(total_ref, left_ref, ortho_ref, right_ref, squares_ref):
    rank = left_ref.shape[1]
    cols = right_ref.shape[1]
    tile = 8
    wide = 2 * rank
    full = total_ref[:, cols : cols + wide]
    row = lax.broadcasted_iota(jnp.int32, (rank, wide), 0)
    lane = lax.broadcasted_iota(jnp.int32, (rank, wide), 1)
    diagonal = jnp.where(lane == row, full, 0.0)
    down = lax.rsqrt(jnp.sum(diagonal, axis=1, keepdims=True))
    along = lax.rsqrt(jnp.sum(diagonal + jnp.where(lane == row + rank, 1.0, 0.0), axis=0, keepdims=True))
    scaled = jnp.where(lane < rank, full * down * along, jnp.where(lane == row + rank, down, 0.0))
    blocks = [scaled[b * tile : (b + 1) * tile, :] for b in range(rank // tile)]
    row_of = lax.broadcasted_iota(jnp.int32, (tile, wide), 0)
    for k in range(0, rank, 2):
        b, r = divmod(k, tile)
        first, second = blocks[b][r : r + 1, :], blocks[b][r + 1 : r + 2, :]
        a, c, d = first[:, k : k + 1], first[:, k + 1 : k + 2], second[:, k + 1 : k + 2]
        det = a * d - c * c
        inv = 1.0 / det
        to_first = (d * inv) * first - (c * inv) * second
        to_second = (a * inv) * second - (c * inv) * first
        unit_first = first * lax.rsqrt(a)
        unit_second = (second - (c / a) * first) * lax.rsqrt(det / a)
        for i in range(b, rank // tile):
            old = blocks[i]
            new = old - old[:, k : k + 1] * to_first - old[:, k + 1 : k + 2] * to_second
            if i == b:
                new = jnp.where(row_of > r + 1, new, old)
                new = jnp.where(row_of == r, unit_first, new)
                new = jnp.where(row_of == r + 1, unit_second, new)
            blocks[i] = new
    inverse = jnp.concatenate(blocks, axis=0)[:, rank:]
    ortho_ref[...] = lax.dot_general(
        left_ref[...], inverse, (((1,), (1,)), ((), ())), precision=HIGH,
        preferred_element_type=jnp.float32,
    )
    right = jnp.dot(
        inverse, total_ref[:, :cols], precision=HIGH, preferred_element_type=jnp.float32
    )
    right_ref[...] = right
    squares = lax.dot_general(
        jnp.ones((tile, cols), jnp.float32), right * right, (((1,), (1,)), ((), ())),
        precision=HIGH, preferred_element_type=jnp.float32,
    )
    squares = jnp.concatenate([squares, squares], axis=1)
    for i in range(squares_ref.shape[0]):
        squares_ref[i] = squares


def finish(ortho_ref, right_ref, squares_ref, factor_ref, update_ref, *, scale):
    rank = ortho_ref.shape[1]
    squares = squares_ref[0]
    for i in range(1, squares_ref.shape[0]):
        squares = squares + squares_ref[i]
    root = jnp.sqrt(squares[:1, :rank] + 1e-06)
    row = lax.broadcasted_iota(jnp.int32, (rank, rank), 0)
    lane = lax.broadcasted_iota(jnp.int32, (rank, rank), 1)
    root = jnp.sum(jnp.where(row == lane, root, 0.0), axis=1, keepdims=True)
    factor = right_ref[...] / root
    factor_ref[...] = factor
    update = jnp.dot(ortho_ref[...], factor, precision=HIGH, preferred_element_type=jnp.float32)
    update_ref[...] = (scale * update).astype(update_ref.dtype)


def local_kernel(kernel, *out_shapes):
    return pl.pallas_call(
        kernel,
        out_shape=out_shapes,
        compiler_params=pltpu.CompilerParams(vmem_limit_bytes=4 * 1024 * 1024),
    )


def body(inputs, cotangent, momentum, right_prev):
    out_total = cotangent.shape[1]
    shards = lax.axis_size(SHARD)
    in_total = momentum.shape[1] * shards
    rank = right_prev.shape[1]
    rows, cols = momentum.shape
    blended = momentum + jnp.sum(gradient_rows(inputs, cotangent), axis=0)
    left_part = jnp.dot(blended, right_prev, precision=HIGH)
    packed = jnp.concatenate([left_part[: rows // 2], left_part[rows // 2 :]], axis=1)
    packed = jnp.sum(from_everyone(packed, SHARD), axis=0)
    left_raw = jnp.concatenate([packed[:, :rank], packed[:, rank:]], axis=0)
    both = jnp.concatenate([blended, left_raw, jnp.zeros_like(left_raw)], axis=1)
    total = rep_total(lax.dot_general(left_raw, both, (((0,), (0,)), ((), ())), precision=HIGH))
    f32 = functools.partial(jax.ShapeDtypeStruct, dtype=jnp.float32)
    ortho, right_rows, squares = local_kernel(
        eliminate, f32((rows, rank)), f32((rank, cols)), f32((shards, 8, 2 * rank))
    )(total, left_raw)
    squares = exchanged(squares, SHARD)
    new_momentum = blended - 0.05 * jnp.dot(ortho, right_rows, precision=HIGH)
    scale = (out_total * in_total / rank) ** 0.5
    factor_rows, update = local_kernel(
        functools.partial(finish, scale=scale),
        f32((rank, cols)), jax.ShapeDtypeStruct((rows, cols), jnp.bfloat16),
    )(ortho, right_rows, squares)
    return (new_momentum, factor_rows.T, update)


def solution(mesh):
    finer = Mesh(mesh.devices.reshape(4, 12, 2, mesh.shape["shard"]), (*REP, SHARD))
    in_specs = (P(REP, SHARD), P(REP, None), P(REP, SHARD), P(SHARD, None))
    out_specs = (P(REP, SHARD), P(SHARD, None), P(REP, SHARD))
    return jax.shard_map(body, mesh=finer, in_specs=in_specs, out_specs=out_specs, check_vma=False)
```

```python
import functools

import jax
import jax.numpy as jnp
from jax import lax
from jax.experimental import pallas as pl
from jax.experimental.pallas import tpu as pltpu
from jax.sharding import Mesh
from jax.sharding import PartitionSpec as P

X, Z, CORE, SHARD = "rep_x", "rep_z", "rep_core", "shard"
REP = (X, Z, CORE)
CLASSES = 3
HIGH = lax.Precision.HIGHEST


def exchanged(pieces, axis, groups=None):
    return lax.all_to_all(pieces, axis, 0, 0, tiled=True, axis_index_groups=groups)


def from_everyone(value, axis):
    count = lax.axis_size(axis)
    return exchanged(jnp.broadcast_to(value[None], (count, *value.shape)), axis)


def sent(value, axis, distance):
    size = lax.axis_size(axis)
    return lax.ppermute(value, axis, [(i, (i + distance) % size) for i in range(size)])


def gated(value, *earlier):
    return lax.optimization_barrier((value, *earlier))[0]


def gradient_rows(inputs, cotangent):
    nx, nz = lax.axis_size(X), lax.axis_size(Z)
    na, nb = nz // CLASSES, CLASSES
    cols = inputs.shape[1]
    rows = cotangent.shape[1] // (nx * nz * 2)
    x, z, core = lax.axis_index(X), lax.axis_index(Z), lax.axis_index(CORE)
    half = na * nb * rows // 2

    partial = lax.dot_general(
        cotangent, inputs, (((0,), (0,)), ((), ())), preferred_element_type=jnp.float32
    ).reshape(nx, na, nb, 2, rows, cols)

    def piece(ahead, which):
        at_x = lax.dynamic_index_in_dim(partial, (x + ahead) % nx, 0, keepdims=False)
        return lax.dynamic_index_in_dim(at_x, which, 2, keepdims=False).reshape(-1, cols)

    near = jnp.stack([piece(ahead, 1 - core) for ahead in (1, 3, 0)])
    far, near, mine_far, mine_before, mine_after, mine = lax.optimization_barrier(
        (piece(2, 1 - core), near, *(piece(ahead, core) for ahead in (2, 1, 3, 0)))
    )
    far = sent(far, CORE, 1)
    near = sent(near, CORE, 1)
    far_up, far_down = mine_far[:half] + far[:half], mine_far[half:] + far[half:]
    relay_up = sent(far_up, X, 1)
    relay_down = sent(far_down, X, -1)
    near = gated(near, far_up, far_down)
    before_low = mine_before[:half] + near[0, :half]
    before_high = mine_before[half:] + near[0, half:]
    after_low = mine_after[:half] + near[1, :half]
    after_high = mine_after[half:] + near[1, half:]
    high_below = sent(before_high, X, 1)
    low_above = sent(after_low, X, -1)
    relay_up = gated(relay_up, before_low, before_high, after_low)
    low_below = sent(before_low + relay_up, X, 1)
    relay_down = gated(relay_down, after_high, before_high, after_low)
    high_above = sent(after_high + relay_down, X, -1)
    own = lax.optimization_barrier(mine + near[2])
    low = own[:half] + low_below + low_above
    high = own[half:] + high_below + high_above
    over_x = jnp.concatenate([low, high], axis=0).reshape(na, nb, rows, cols)

    kind = z % nb

    def of_class(ahead):
        return lax.dynamic_index_in_dim(over_x, (kind + ahead) % nb, 1, keepdims=False)

    up = sent(of_class(1), Z, 1)
    down = sent(of_class(nb - 1), Z, -1)
    over_near_z = of_class(0) + up + down
    groups = [[a * nb + b for a in range(na)] for b in range(nb)]
    return exchanged(over_near_z, Z, groups)


def rep_total(value):
    members = lax.axis_size((X, CORE))
    piece = value.reshape(members, value.shape[0] // members, value.shape[1])
    piece = jnp.sum(exchanged(piece, (X, CORE)), axis=0)
    piece = jnp.sum(from_everyone(piece, Z), axis=0)
    return from_everyone(piece, (X, CORE)).reshape(value.shape)


def eliminate(total_ref, left_ref, ortho_ref, right_ref, squares_ref):
    rank = left_ref.shape[1]
    cols = right_ref.shape[1]
    tile = 8
    wide = 2 * rank
    full = total_ref[:, cols : cols + wide]
    row = lax.broadcasted_iota(jnp.int32, (rank, wide), 0)
    lane = lax.broadcasted_iota(jnp.int32, (rank, wide), 1)
    diagonal = jnp.where(lane == row, full, 0.0)
    down = lax.rsqrt(jnp.sum(diagonal, axis=1, keepdims=True))
    along = lax.rsqrt(jnp.sum(diagonal + jnp.where(lane == row + rank, 1.0, 0.0), axis=0, keepdims=True))
    scaled = jnp.where(lane < rank, full * down * along, jnp.where(lane == row + rank, down, 0.0))
    blocks = [scaled[b * tile : (b + 1) * tile, :] for b in range(rank // tile)]
    row_of = lax.broadcasted_iota(jnp.int32, (tile, wide), 0)
    full_tile = functools.partial(jnp.broadcast_to, shape=(tile, wide))
    for k in range(0, rank, 2):
        b, r = divmod(k, tile)
        first, second = full_tile(blocks[b][r : r + 1, :]), full_tile(blocks[b][r + 1 : r + 2, :])
        a, c = full_tile(first[:, k : k + 1]), full_tile(first[:, k + 1 : k + 2])
        d = full_tile(second[:, k + 1 : k + 2])
        det = a * d - c * c
        inv = 1.0 / det
        to_first = (d * first - c * second) * inv
        to_second = (a * second - c * first) * inv
        for i in range(b, rank // tile):
            old = blocks[i]
            new = old - full_tile(old[:, k : k + 1]) * to_first
            new = new - full_tile(old[:, k + 1 : k + 2]) * to_second
            if i == b:
                root = lax.rsqrt(a)
                new = jnp.where(row_of > r + 1, new, old)
                new = jnp.where(row_of == r, first * root, new)
                new = jnp.where(row_of == r + 1, (a * second - c * first) * (root * lax.rsqrt(det)), new)
            blocks[i] = new
    inverse = jnp.concatenate(blocks, axis=0)[:, rank:]
    ortho_ref[...] = lax.dot_general(
        left_ref[...], inverse, (((1,), (1,)), ((), ())), precision=HIGH,
        preferred_element_type=jnp.float32,
    )
    right = jnp.dot(
        inverse, total_ref[:, :cols], precision=HIGH, preferred_element_type=jnp.float32
    )
    right_ref[...] = right
    squares = lax.dot_general(
        jnp.ones((tile, cols), jnp.float32), right * right, (((1,), (1,)), ((), ())),
        precision=HIGH, preferred_element_type=jnp.float32,
    )
    squares = jnp.concatenate([squares, squares], axis=1)
    for i in range(squares_ref.shape[0]):
        squares_ref[i] = squares


def blend(pieces_ref, momentum_ref, right_ref, blended_ref, packed_ref):
    blended = momentum_ref[...]
    for i in range(pieces_ref.shape[0]):
        blended = blended + pieces_ref[i]
    blended_ref[...] = blended
    left = lax.dot_general(
        blended, right_ref[...], (((1,), (1,)), ((), ())), precision=HIGH,
        preferred_element_type=jnp.float32,
    )
    half = left.shape[0] // 2
    packed = jnp.concatenate([left[:half], left[half:]], axis=1)
    for i in range(packed_ref.shape[0]):
        packed_ref[i] = packed


def project(packed_ref, blended_ref, left_ref, value_ref):
    packed = packed_ref[0]
    for i in range(1, packed_ref.shape[0]):
        packed = packed + packed_ref[i]
    rank = left_ref.shape[1]
    left = jnp.concatenate([packed[:, :rank], packed[:, rank:]], axis=0)
    left_ref[...] = left
    both = jnp.concatenate([blended_ref[...], left, left], axis=1)
    value_ref[...] = lax.dot_general(
        left, both, (((0,), (0,)), ((), ())), precision=HIGH, preferred_element_type=jnp.float32
    )


def finish(ortho_ref, right_ref, squares_ref, blended_ref, momentum_ref, factor_ref, update_ref, *, scale):
    rank = ortho_ref.shape[1]
    squares = squares_ref[0]
    for i in range(1, squares_ref.shape[0]):
        squares = squares + squares_ref[i]
    root = jnp.sqrt(squares[:1, :rank] + 1e-06)
    row = lax.broadcasted_iota(jnp.int32, (rank, rank), 0)
    lane = lax.broadcasted_iota(jnp.int32, (rank, rank), 1)
    root = jnp.sum(jnp.where(row == lane, root, 0.0), axis=1, keepdims=True)
    right = right_ref[...]
    factor = right / root
    factor_ref[...] = factor
    ortho = ortho_ref[...]
    dot = functools.partial(jnp.dot, precision=HIGH, preferred_element_type=jnp.float32)
    momentum_ref[...] = blended_ref[...] - 0.05 * dot(ortho, right)
    update_ref[...] = (scale * dot(ortho, factor)).astype(update_ref.dtype)


def local_kernel(kernel, *out_shapes):
    return pl.pallas_call(
        kernel,
        out_shape=out_shapes,
        compiler_params=pltpu.CompilerParams(vmem_limit_bytes=4 * 1024 * 1024),
    )


def body(inputs, cotangent, momentum, right_prev):
    out_total = cotangent.shape[1]
    shards = lax.axis_size(SHARD)
    in_total = momentum.shape[1] * shards
    rank = right_prev.shape[1]
    rows, cols = momentum.shape
    f32 = functools.partial(jax.ShapeDtypeStruct, dtype=jnp.float32)
    pieces = gradient_rows(inputs, cotangent)
    blended, packed = local_kernel(
        blend, f32((rows, cols)), f32((shards, rows // 2, 2 * rank))
    )(pieces, momentum, right_prev.T)
    left_raw, value = local_kernel(
        project, f32((rows, rank)), f32((rank, cols + 2 * rank))
    )(exchanged(packed, SHARD), blended)
    ortho, right_rows, squares = local_kernel(
        eliminate, f32((rows, rank)), f32((rank, cols)), f32((shards, 8, 2 * rank))
    )(rep_total(value), left_raw)
    scale = (out_total * in_total / rank) ** 0.5
    new_momentum, factor_rows, update = local_kernel(
        functools.partial(finish, scale=scale),
        f32((rows, cols)), f32((rank, cols)), jax.ShapeDtypeStruct((rows, cols), jnp.bfloat16),
    )(ortho, right_rows, exchanged(squares, SHARD), blended)
    return (new_momentum, factor_rows.T, update)


def solution(mesh):
    finer = Mesh(mesh.devices.reshape(4, 12, 2, mesh.shape["shard"]), (*REP, SHARD))
    in_specs = (P(REP, SHARD), P(REP, None), P(REP, SHARD), P(SHARD, None))
    out_specs = (P(REP, SHARD), P(SHARD, None), P(REP, SHARD))
    return jax.shard_map(body, mesh=finer, in_specs=in_specs, out_specs=out_specs, check_vma=False)
```

```python
import functools

import jax
import jax.numpy as jnp
from jax import lax
from jax.experimental import pallas as pl
from jax.experimental.pallas import tpu as pltpu
from jax.sharding import Mesh
from jax.sharding import PartitionSpec as P

X, Z, CORE, SHARD = "rep_x", "rep_z", "rep_core", "shard"
REP = (X, Z, CORE)
CLASSES = 3
HIGH = lax.Precision.HIGHEST


def exchanged(pieces, axis, groups=None):
    return lax.all_to_all(pieces, axis, 0, 0, tiled=True, axis_index_groups=groups)


def from_everyone(value, axis):
    count = lax.axis_size(axis)
    return exchanged(jnp.broadcast_to(value[None], (count, *value.shape)), axis)


def sent(value, axis, distance):
    size = lax.axis_size(axis)
    return lax.ppermute(value, axis, [(i, (i + distance) % size) for i in range(size)])


def gated(value, *earlier):
    return lax.optimization_barrier((value, *earlier))[0]


def gradient_rows(inputs, cotangent):
    nx, nz = lax.axis_size(X), lax.axis_size(Z)
    na, nb = nz // CLASSES, CLASSES
    cols = inputs.shape[1]
    rows = cotangent.shape[1] // (nx * nz * 2)
    x, z, core = lax.axis_index(X), lax.axis_index(Z), lax.axis_index(CORE)
    half = na * nb * rows * 7 // 12 // 8 * 8

    partial = lax.dot_general(
        cotangent, inputs, (((0,), (0,)), ((), ())), preferred_element_type=jnp.float32
    ).reshape(nx, na, nb, 2, rows, cols)

    def piece(ahead, which):
        at_x = lax.dynamic_index_in_dim(partial, (x + ahead) % nx, 0, keepdims=False)
        return lax.dynamic_index_in_dim(at_x, which, 2, keepdims=False).reshape(-1, cols)

    near = jnp.stack([piece(ahead, 1 - core) for ahead in (1, 3, 0)])
    far, near, mine_far, mine_before, mine_after, mine = lax.optimization_barrier(
        (piece(2, 1 - core), near, *(piece(ahead, core) for ahead in (2, 1, 3, 0)))
    )
    far = sent(far, CORE, 1)
    near = sent(near, CORE, 1)
    far_up, far_down = mine_far[:half] + far[:half], mine_far[half:] + far[half:]
    relay_up = sent(far_up, X, 1)
    relay_down = sent(far_down, X, -1)
    near = gated(near, far_up, far_down)
    before_high = mine_before[half:] + near[0, half:]
    after_low = mine_after[:half] + near[1, :half]
    high_below = sent(before_high, X, 1)
    low_above = sent(after_low, X, -1)
    near = gated(near, before_high, after_low)
    own_low = lax.optimization_barrier(mine[:half] + near[2, :half])
    near = gated(near, own_low)
    before_low = lax.optimization_barrier(mine_before[:half] + near[0, :half] + relay_up)
    low_below = sent(before_low, X, 1)
    near = gated(near, before_low)
    own_high = lax.optimization_barrier(mine[half:] + near[2, half:])
    near = gated(near, own_high)
    after_high = lax.optimization_barrier(mine_after[half:] + near[1, half:] + relay_down)
    high_above = sent(after_high, X, -1)
    low = own_low + low_below + low_above
    high = own_high + high_below + high_above
    over_x = jnp.concatenate([low, high], axis=0).reshape(na, nb, rows, cols)

    kind = z % nb

    def of_class(ahead):
        return lax.dynamic_index_in_dim(over_x, (kind + ahead) % nb, 1, keepdims=False)

    up = sent(of_class(1), Z, 1)
    down = sent(of_class(nb - 1), Z, -1)
    over_near_z = of_class(0) + up + down
    groups = [[a * nb + b for a in range(na)] for b in range(nb)]
    return exchanged(over_near_z, Z, groups)


def rep_total(value):
    members = lax.axis_size((X, CORE))
    piece = value.reshape(members, value.shape[0] // members, value.shape[1])
    piece = jnp.sum(exchanged(piece, (X, CORE)), axis=0)
    piece = jnp.sum(from_everyone(piece, Z), axis=0)
    return from_everyone(piece, (X, CORE)).reshape(value.shape)


def eliminate(total_ref, left_ref, ortho_ref, right_ref, squares_ref):
    rank = left_ref.shape[1]
    cols = right_ref.shape[1]
    tile = 8
    wide = 2 * rank
    full = total_ref[:, cols : cols + wide]
    row = lax.broadcasted_iota(jnp.int32, (rank, wide), 0)
    lane = lax.broadcasted_iota(jnp.int32, (rank, wide), 1)
    diagonal = jnp.where(lane == row, full, 0.0)
    down = lax.rsqrt(jnp.sum(diagonal, axis=1, keepdims=True))
    along = lax.rsqrt(jnp.sum(diagonal + jnp.where(lane == row + rank, 1.0, 0.0), axis=0, keepdims=True))
    scaled = jnp.where(lane < rank, full * down * along, jnp.where(lane == row + rank, down, 0.0))
    blocks = [scaled[b * tile : (b + 1) * tile, :] for b in range(rank // tile)]
    row_of = lax.broadcasted_iota(jnp.int32, (tile, wide), 0)
    full_tile = functools.partial(jnp.broadcast_to, shape=(tile, wide))
    for k in range(0, rank, 2):
        b, r = divmod(k, tile)
        first, second = full_tile(blocks[b][r : r + 1, :]), full_tile(blocks[b][r + 1 : r + 2, :])
        a, c = full_tile(first[:, k : k + 1]), full_tile(first[:, k + 1 : k + 2])
        d = full_tile(second[:, k + 1 : k + 2])
        det = a * d - c * c
        inv = 1.0 / det
        to_first = (d * first - c * second) * inv
        to_second = (a * second - c * first) * inv
        for i in range(b, rank // tile):
            old = blocks[i]
            new = old - full_tile(old[:, k : k + 1]) * to_first
            new = new - full_tile(old[:, k + 1 : k + 2]) * to_second
            if i == b:
                root = lax.rsqrt(a)
                new = jnp.where(row_of > r + 1, new, old)
                new = jnp.where(row_of == r, first * root, new)
                new = jnp.where(row_of == r + 1, (a * second - c * first) * (root * lax.rsqrt(det)), new)
            blocks[i] = new
    inverse = jnp.concatenate(blocks, axis=0)[:, rank:]
    ortho_ref[...] = lax.dot_general(
        left_ref[...], inverse, (((1,), (1,)), ((), ())), precision=HIGH,
        preferred_element_type=jnp.float32,
    )
    right = jnp.dot(
        inverse, total_ref[:, :cols], precision=HIGH, preferred_element_type=jnp.float32
    )
    right_ref[...] = right
    squares = lax.dot_general(
        jnp.ones((tile, cols), jnp.float32), right * right, (((1,), (1,)), ((), ())),
        precision=HIGH, preferred_element_type=jnp.float32,
    )
    squares = jnp.concatenate([squares, squares], axis=1)
    for i in range(squares_ref.shape[0]):
        squares_ref[i] = squares


def blend(pieces_ref, momentum_ref, right_ref, blended_ref, packed_ref):
    blended = momentum_ref[...]
    for i in range(pieces_ref.shape[0]):
        blended = blended + pieces_ref[i]
    blended_ref[...] = blended
    left = lax.dot_general(
        blended, right_ref[...], (((1,), (1,)), ((), ())), precision=HIGH,
        preferred_element_type=jnp.float32,
    )
    half = left.shape[0] // 2
    packed = jnp.concatenate([left[:half], left[half:]], axis=1)
    for i in range(packed_ref.shape[0]):
        packed_ref[i] = packed


def project(packed_ref, blended_ref, left_ref, value_ref):
    packed = packed_ref[0]
    for i in range(1, packed_ref.shape[0]):
        packed = packed + packed_ref[i]
    rank = left_ref.shape[1]
    left = jnp.concatenate([packed[:, :rank], packed[:, rank:]], axis=0)
    left_ref[...] = left
    both = jnp.concatenate([blended_ref[...], left, left], axis=1)
    value_ref[...] = lax.dot_general(
        left, both, (((0,), (0,)), ((), ())), precision=HIGH, preferred_element_type=jnp.float32
    )


def finish(ortho_ref, right_ref, squares_ref, blended_ref, momentum_ref, factor_ref, update_ref, *, scale):
    rank = ortho_ref.shape[1]
    squares = squares_ref[0]
    for i in range(1, squares_ref.shape[0]):
        squares = squares + squares_ref[i]
    root = jnp.sqrt(squares[:1, :rank] + 1e-06)
    row = lax.broadcasted_iota(jnp.int32, (rank, rank), 0)
    lane = lax.broadcasted_iota(jnp.int32, (rank, rank), 1)
    root = jnp.sum(jnp.where(row == lane, root, 0.0), axis=1, keepdims=True)
    right = right_ref[...]
    factor = right / root
    factor_ref[...] = factor
    ortho = ortho_ref[...]
    dot = functools.partial(jnp.dot, precision=HIGH, preferred_element_type=jnp.float32)
    momentum_ref[...] = blended_ref[...] - 0.05 * dot(ortho, right)
    update_ref[...] = (scale * dot(ortho, factor)).astype(update_ref.dtype)


def local_kernel(kernel, *out_shapes):
    return pl.pallas_call(
        kernel,
        out_shape=out_shapes,
        compiler_params=pltpu.CompilerParams(vmem_limit_bytes=4 * 1024 * 1024),
    )


def body(inputs, cotangent, momentum, right_prev):
    out_total = cotangent.shape[1]
    shards = lax.axis_size(SHARD)
    in_total = momentum.shape[1] * shards
    rank = right_prev.shape[1]
    rows, cols = momentum.shape
    f32 = functools.partial(jax.ShapeDtypeStruct, dtype=jnp.float32)
    pieces = gradient_rows(inputs, cotangent)
    blended, packed = local_kernel(
        blend, f32((rows, cols)), f32((shards, rows // 2, 2 * rank))
    )(pieces, momentum, right_prev.T)
    left_raw, value = local_kernel(
        project, f32((rows, rank)), f32((rank, cols + 2 * rank))
    )(exchanged(packed, SHARD), blended)
    ortho, right_rows, squares = local_kernel(
        eliminate, f32((rows, rank)), f32((rank, cols)), f32((shards, 8, 2 * rank))
    )(rep_total(value), left_raw)
    scale = (out_total * in_total / rank) ** 0.5
    new_momentum, factor_rows, update = local_kernel(
        functools.partial(finish, scale=scale),
        f32((rows, cols)), f32((rank, cols)), jax.ShapeDtypeStruct((rows, cols), jnp.bfloat16),
    )(ortho, right_rows, exchanged(squares, SHARD), blended)
    return (new_momentum, factor_rows.T, update)


def solution(mesh):
    finer = Mesh(mesh.devices.reshape(4, 12, 2, mesh.shape["shard"]), (*REP, SHARD))
    in_specs = (P(REP, SHARD), P(REP, None), P(REP, SHARD), P(SHARD, None))
    out_specs = (P(REP, SHARD), P(SHARD, None), P(REP, SHARD))
    return jax.shard_map(body, mesh=finer, in_specs=in_specs, out_specs=out_specs, check_vma=False)
```

```python
import functools

import jax
import jax.numpy as jnp
from jax import lax
from jax.experimental import pallas as pl
from jax.experimental.pallas import tpu as pltpu
from jax.sharding import Mesh
from jax.sharding import PartitionSpec as P

X, Z, CORE, SHARD = "rep_x", "rep_z", "rep_core", "shard"
REP = (X, Z, CORE)
CLASSES = 3
HIGH = lax.Precision.HIGHEST


def exchanged(pieces, axis, groups=None):
    return lax.all_to_all(pieces, axis, 0, 0, tiled=True, axis_index_groups=groups)


def from_everyone(value, axis):
    count = lax.axis_size(axis)
    return exchanged(jnp.broadcast_to(value[None], (count, *value.shape)), axis)


def sent(value, axis, distance):
    size = lax.axis_size(axis)
    return lax.ppermute(value, axis, [(i, (i + distance) % size) for i in range(size)])


def gated(value, *earlier):
    return lax.optimization_barrier((value, *earlier))[0]


def gradient_rows(inputs, cotangent):
    nx, nz = lax.axis_size(X), lax.axis_size(Z)
    na, nb = nz // CLASSES, CLASSES
    cols = inputs.shape[1]
    rows = cotangent.shape[1] // (nx * nz * 2)
    x, z, core = lax.axis_index(X), lax.axis_index(Z), lax.axis_index(CORE)
    half = na * nb * rows * 13 // 24 // 8 * 8

    partial = lax.dot_general(
        cotangent, inputs, (((0,), (0,)), ((), ())), preferred_element_type=jnp.float32
    ).reshape(nx, na, nb, 2, rows, cols)

    def piece(ahead, which):
        at_x = lax.dynamic_index_in_dim(partial, (x + ahead) % nx, 0, keepdims=False)
        return lax.dynamic_index_in_dim(at_x, which, 2, keepdims=False).reshape(-1, cols)

    near = jnp.stack([piece(ahead, 1 - core) for ahead in (1, 3, 0)])
    far, near, mine_far, mine_before, mine_after, mine = lax.optimization_barrier(
        (piece(2, 1 - core), near, *(piece(ahead, core) for ahead in (2, 1, 3, 0)))
    )
    far = sent(far, CORE, 1)
    near = sent(near, CORE, 1)
    far_up, far_down = mine_far[:half] + far[:half], mine_far[half:] + far[half:]
    relay_up = sent(far_up, X, 1)
    relay_down = sent(far_down, X, -1)
    near = gated(near, far_up, far_down)
    before_high = mine_before[half:] + near[0, half:]
    after_low = mine_after[:half] + near[1, :half]
    high_below = sent(before_high, X, 1)
    low_above = sent(after_low, X, -1)
    near = gated(near, before_high, after_low)
    own_low = lax.optimization_barrier(mine[:half] + near[2, :half])
    near = gated(near, own_low)
    before_low = lax.optimization_barrier(mine_before[:half] + near[0, :half] + relay_up)
    low_below = sent(before_low, X, 1)
    near = gated(near, before_low)
    own_high = lax.optimization_barrier(mine[half:] + near[2, half:])
    near = gated(near, own_high)
    after_high = lax.optimization_barrier(mine_after[half:] + near[1, half:] + relay_down)
    high_above = sent(after_high, X, -1)
    low = own_low + low_below + low_above
    high = own_high + high_below + high_above
    over_x = jnp.concatenate([low, high], axis=0).reshape(na, nb, rows, cols)

    kind = z % nb

    def of_class(ahead):
        return lax.dynamic_index_in_dim(over_x, (kind + ahead) % nb, 1, keepdims=False)

    up = sent(of_class(1), Z, 1)
    down = sent(of_class(nb - 1), Z, -1)
    over_near_z = of_class(0) + up + down
    groups = [[a * nb + b for a in range(na)] for b in range(nb)]
    return exchanged(over_near_z, Z, groups)


def rep_total(value):
    members = lax.axis_size((X, CORE))
    piece = value.reshape(members, value.shape[0] // members, value.shape[1])
    piece = jnp.sum(exchanged(piece, (X, CORE)), axis=0)
    piece = jnp.sum(from_everyone(piece, Z), axis=0)
    return from_everyone(piece, (X, CORE)).reshape(value.shape)


def eliminate(total_ref, left_ref, ortho_ref, right_ref, squares_ref):
    rank = left_ref.shape[1]
    cols = right_ref.shape[1]
    tile = 8
    wide = 2 * rank
    full = total_ref[:, cols : cols + wide]
    row = lax.broadcasted_iota(jnp.int32, (rank, wide), 0)
    lane = lax.broadcasted_iota(jnp.int32, (rank, wide), 1)
    diagonal = jnp.where(lane == row, full, 0.0)
    down = lax.rsqrt(jnp.sum(diagonal, axis=1, keepdims=True))
    along = lax.rsqrt(jnp.sum(diagonal + jnp.where(lane == row + rank, 1.0, 0.0), axis=0, keepdims=True))
    scaled = jnp.where(lane < rank, full * down * along, jnp.where(lane == row + rank, down, 0.0))
    blocks = [scaled[b * tile : (b + 1) * tile, :] for b in range(rank // tile)]
    row_of = lax.broadcasted_iota(jnp.int32, (tile, wide), 0)
    full_tile = functools.partial(jnp.broadcast_to, shape=(tile, wide))
    for k in range(0, rank, 4):
        b, r = divmod(k, tile)
        r0, r1, r2, r3 = (full_tile(blocks[b][r + i : r + i + 1, :]) for i in range(4))

        def at(row, j, k=k):
            return full_tile(row[:, k + j : k + j + 1])

        e00, e01, e02, e03 = (at(r0, j) for j in range(4))
        e11, e12, e13 = (at(r1, j) for j in range(1, 4))
        e22, e23, e33 = at(r2, 2), at(r2, 3), at(r3, 3)
        det = e00 * e11 - e01 * e01
        inv = 1.0 / det
        s0, s1 = e11 * r0 - e01 * r1, e00 * r1 - e01 * r0
        u02, u03 = (e11 * e02 - e01 * e12) * inv, (e11 * e03 - e01 * e13) * inv
        u12, u13 = (e00 * e12 - e01 * e02) * inv, (e00 * e13 - e01 * e03) * inv
        f22 = e22 - e02 * u02 - e12 * u12
        f23 = e23 - e02 * u03 - e12 * u13
        f33 = e33 - e03 * u03 - e13 * u13
        t0, t1 = s0 * inv, s1 * inv
        r2, r3 = r2 - e02 * t0 - e12 * t1, r3 - e03 * t0 - e13 * t1
        second = f22 * f33 - f23 * f23
        inv = 1.0 / second
        s3 = f22 * r3 - f23 * r2
        t2, t3 = (f33 * r2 - f23 * r3) * inv, s3 * inv
        t0, t1 = t0 - u02 * t2 - u03 * t3, t1 - u12 * t2 - u13 * t3
        for i in range(b, rank // tile):
            old = blocks[i]
            new = (old - at(old, 0) * t0 - at(old, 1) * t1) - (at(old, 2) * t2 + at(old, 3) * t3)
            if i == b:
                root, later = lax.rsqrt(e00), lax.rsqrt(f22)
                new = jnp.where(row_of > r + 3, new, old)
                new = jnp.where(row_of == r, r0 * root, new)
                new = jnp.where(row_of == r + 1, s1 * (root * lax.rsqrt(det)), new)
                new = jnp.where(row_of == r + 2, r2 * later, new)
                new = jnp.where(row_of == r + 3, s3 * (later * lax.rsqrt(second)), new)
            blocks[i] = new
    inverse = jnp.concatenate(blocks, axis=0)[:, rank:]
    ortho_ref[...] = lax.dot_general(
        left_ref[...], inverse, (((1,), (1,)), ((), ())), precision=HIGH,
        preferred_element_type=jnp.float32,
    )
    right = jnp.dot(
        inverse, total_ref[:, :cols], precision=HIGH, preferred_element_type=jnp.float32
    )
    right_ref[...] = right
    squares = lax.dot_general(
        jnp.ones((tile, cols), jnp.float32), right * right, (((1,), (1,)), ((), ())),
        precision=HIGH, preferred_element_type=jnp.float32,
    )
    squares = jnp.concatenate([squares, squares], axis=1)
    for i in range(squares_ref.shape[0]):
        squares_ref[i] = squares


def blend(pieces_ref, momentum_ref, right_ref, blended_ref, packed_ref):
    blended = momentum_ref[...]
    for i in range(pieces_ref.shape[0]):
        blended = blended + pieces_ref[i]
    blended_ref[...] = blended
    left = lax.dot_general(
        blended, right_ref[...], (((1,), (1,)), ((), ())), precision=HIGH,
        preferred_element_type=jnp.float32,
    )
    half = left.shape[0] // 2
    packed = jnp.concatenate([left[:half], left[half:]], axis=1)
    for i in range(packed_ref.shape[0]):
        packed_ref[i] = packed


def project(packed_ref, blended_ref, left_ref, value_ref):
    packed = packed_ref[0]
    for i in range(1, packed_ref.shape[0]):
        packed = packed + packed_ref[i]
    rank = left_ref.shape[1]
    left = jnp.concatenate([packed[:, :rank], packed[:, rank:]], axis=0)
    left_ref[...] = left
    both = jnp.concatenate([blended_ref[...], left, left], axis=1)
    value_ref[...] = lax.dot_general(
        left, both, (((0,), (0,)), ((), ())), precision=HIGH, preferred_element_type=jnp.float32
    )


def finish(ortho_ref, right_ref, squares_ref, blended_ref, momentum_ref, factor_ref, update_ref, *, scale):
    rank = ortho_ref.shape[1]
    squares = squares_ref[0]
    for i in range(1, squares_ref.shape[0]):
        squares = squares + squares_ref[i]
    root = jnp.sqrt(squares[:1, :rank] + 1e-06)
    row = lax.broadcasted_iota(jnp.int32, (rank, rank), 0)
    lane = lax.broadcasted_iota(jnp.int32, (rank, rank), 1)
    root = jnp.sum(jnp.where(row == lane, root, 0.0), axis=1, keepdims=True)
    right = right_ref[...]
    factor = right / root
    factor_ref[...] = factor
    ortho = ortho_ref[...]
    dot = functools.partial(jnp.dot, precision=HIGH, preferred_element_type=jnp.float32)
    momentum_ref[...] = blended_ref[...] - 0.05 * dot(ortho, right)
    update_ref[...] = (scale * dot(ortho, factor)).astype(update_ref.dtype)


def local_kernel(kernel, *out_shapes):
    return pl.pallas_call(
        kernel,
        out_shape=out_shapes,
        compiler_params=pltpu.CompilerParams(vmem_limit_bytes=4 * 1024 * 1024),
    )


def body(inputs, cotangent, momentum, right_prev):
    out_total = cotangent.shape[1]
    shards = lax.axis_size(SHARD)
    in_total = momentum.shape[1] * shards
    rank = right_prev.shape[1]
    rows, cols = momentum.shape
    f32 = functools.partial(jax.ShapeDtypeStruct, dtype=jnp.float32)
    pieces = gradient_rows(inputs, cotangent)
    blended, packed = local_kernel(
        blend, f32((rows, cols)), f32((shards, rows // 2, 2 * rank))
    )(pieces, momentum, right_prev.T)
    left_raw, value = local_kernel(
        project, f32((rows, rank)), f32((rank, cols + 2 * rank))
    )(exchanged(packed, SHARD), blended)
    ortho, right_rows, squares = local_kernel(
        eliminate, f32((rows, rank)), f32((rank, cols)), f32((shards, 8, 2 * rank))
    )(rep_total(value), left_raw)
    scale = (out_total * in_total / rank) ** 0.5
    new_momentum, factor_rows, update = local_kernel(
        functools.partial(finish, scale=scale),
        f32((rows, cols)), f32((rank, cols)), jax.ShapeDtypeStruct((rows, cols), jnp.bfloat16),
    )(ortho, right_rows, exchanged(squares, SHARD), blended)
    return (new_momentum, factor_rows.T, update)


def solution(mesh):
    finer = Mesh(mesh.devices.reshape(4, 12, 2, mesh.shape["shard"]), (*REP, SHARD))
    in_specs = (P(REP, SHARD), P(REP, None), P(REP, SHARD), P(SHARD, None))
    out_specs = (P(REP, SHARD), P(SHARD, None), P(REP, SHARD))
    return jax.shard_map(body, mesh=finer, in_specs=in_specs, out_specs=out_specs, check_vma=False)
```

```python
import functools

import jax
import jax.numpy as jnp
from jax import lax
from jax.experimental import pallas as pl
from jax.experimental.pallas import tpu as pltpu
from jax.sharding import Mesh
from jax.sharding import PartitionSpec as P

X, Z, CORE, SHARD = "rep_x", "rep_z", "rep_core", "shard"
REP = (X, Z, CORE)
CLASSES = 3
HIGH = lax.Precision.HIGHEST


def exchanged(pieces, axis, groups=None):
    return lax.all_to_all(pieces, axis, 0, 0, tiled=True, axis_index_groups=groups)


def from_everyone(value, axis):
    count = lax.axis_size(axis)
    return exchanged(jnp.broadcast_to(value[None], (count, *value.shape)), axis)


def sent(value, axis, distance):
    size = lax.axis_size(axis)
    return lax.ppermute(value, axis, [(i, (i + distance) % size) for i in range(size)])


def gated(value, *earlier):
    return lax.optimization_barrier((value, *earlier))[0]


def gradient_rows(inputs, cotangent):
    nx, nz = lax.axis_size(X), lax.axis_size(Z)
    na, nb = nz // CLASSES, CLASSES
    cols = inputs.shape[1]
    rows = cotangent.shape[1] // (nx * nz * 2)
    x, z, core = lax.axis_index(X), lax.axis_index(Z), lax.axis_index(CORE)
    half = na * nb * rows * 7 // 12 // 8 * 8

    partial = lax.dot_general(
        cotangent, inputs, (((0,), (0,)), ((), ())), preferred_element_type=jnp.float32
    ).reshape(nx, na, nb, 2, rows, cols)

    def piece(ahead, which):
        at_x = lax.dynamic_index_in_dim(partial, (x + ahead) % nx, 0, keepdims=False)
        return lax.dynamic_index_in_dim(at_x, which, 2, keepdims=False).reshape(-1, cols)

    near = jnp.stack([piece(ahead, 1 - core) for ahead in (1, 3, 0)])
    far, near, mine_far, mine_before, mine_after, mine = lax.optimization_barrier(
        (piece(2, 1 - core), near, *(piece(ahead, core) for ahead in (2, 1, 3, 0)))
    )
    far = sent(far, CORE, 1)
    near = sent(near, CORE, 1)
    far_up, far_down = mine_far[:half] + far[:half], mine_far[half:] + far[half:]
    relay_up = sent(far_up, X, 1)
    relay_down = sent(far_down, X, -1)
    near = gated(near, far_up, far_down)
    before_low = mine_before[:half] + near[0, :half]
    before_high = mine_before[half:] + near[0, half:]
    after_low = mine_after[:half] + near[1, :half]
    after_high = mine_after[half:] + near[1, half:]
    high_below = sent(before_high, X, 1)
    low_above = sent(after_low, X, -1)
    relay_up = gated(relay_up, before_low, before_high, after_low)
    low_below = sent(before_low + relay_up, X, 1)
    relay_down = gated(relay_down, after_high, before_high, after_low)
    high_above = sent(after_high + relay_down, X, -1)
    own = lax.optimization_barrier(mine + near[2])
    low = own[:half] + low_below + low_above
    high = own[half:] + high_below + high_above
    over_x = jnp.concatenate([low, high], axis=0).reshape(na, nb, rows, cols)

    kind = z % nb

    def of_class(ahead):
        return lax.dynamic_index_in_dim(over_x, (kind + ahead) % nb, 1, keepdims=False)

    up = sent(of_class(1), Z, 1)
    down = sent(of_class(nb - 1), Z, -1)
    over_near_z = of_class(0) + up + down
    groups = [[a * nb + b for a in range(na)] for b in range(nb)]
    return exchanged(over_near_z, Z, groups)


def rep_total(value):
    members = lax.axis_size((X, CORE))
    piece = value.reshape(members, value.shape[0] // members, value.shape[1])
    piece = jnp.sum(exchanged(piece, (X, CORE)), axis=0)
    piece = jnp.sum(from_everyone(piece, Z), axis=0)
    return from_everyone(piece, (X, CORE)).reshape(value.shape)


def eliminate(total_ref, left_ref, ortho_ref, right_ref, squares_ref):
    rank = left_ref.shape[1]
    cols = right_ref.shape[1]
    tile = 8
    wide = 2 * rank
    full = total_ref[:, cols : cols + wide]
    row = lax.broadcasted_iota(jnp.int32, (rank, wide), 0)
    lane = lax.broadcasted_iota(jnp.int32, (rank, wide), 1)
    diagonal = jnp.where(lane == row, full, 0.0)
    down = lax.rsqrt(jnp.sum(diagonal, axis=1, keepdims=True))
    along = lax.rsqrt(jnp.sum(diagonal + jnp.where(lane == row + rank, 1.0, 0.0), axis=0, keepdims=True))
    scaled = jnp.where(lane < rank, full * down * along, jnp.where(lane == row + rank, down, 0.0))
    blocks = [scaled[b * tile : (b + 1) * tile, :] for b in range(rank // tile)]
    row_of = lax.broadcasted_iota(jnp.int32, (tile, wide), 0)
    full_tile = functools.partial(jnp.broadcast_to, shape=(tile, wide))
    for k in range(0, rank, 4):
        b, r = divmod(k, tile)
        r0, r1, r2, r3 = (full_tile(blocks[b][r + i : r + i + 1, :]) for i in range(4))

        def at(row, j, k=k):
            return full_tile(row[:, k + j : k + j + 1])

        e00, e01, e02, e03 = (at(r0, j) for j in range(4))
        e11, e12, e13 = (at(r1, j) for j in range(1, 4))
        e22, e23, e33 = at(r2, 2), at(r2, 3), at(r3, 3)
        det = e00 * e11 - e01 * e01
        inv = 1.0 / det
        s0, s1 = e11 * r0 - e01 * r1, e00 * r1 - e01 * r0
        u02, u03 = (e11 * e02 - e01 * e12) * inv, (e11 * e03 - e01 * e13) * inv
        u12, u13 = (e00 * e12 - e01 * e02) * inv, (e00 * e13 - e01 * e03) * inv
        f22 = e22 - e02 * u02 - e12 * u12
        f23 = e23 - e02 * u03 - e12 * u13
        f33 = e33 - e03 * u03 - e13 * u13
        t0, t1 = s0 * inv, s1 * inv
        r2, r3 = r2 - e02 * t0 - e12 * t1, r3 - e03 * t0 - e13 * t1
        second = f22 * f33 - f23 * f23
        inv = 1.0 / second
        s3 = f22 * r3 - f23 * r2
        t2, t3 = (f33 * r2 - f23 * r3) * inv, s3 * inv
        t0, t1 = t0 - u02 * t2 - u03 * t3, t1 - u12 * t2 - u13 * t3
        for i in range(b, rank // tile):
            old = blocks[i]
            new = (old - at(old, 0) * t0 - at(old, 1) * t1) - (at(old, 2) * t2 + at(old, 3) * t3)
            if i == b:
                root, later = lax.rsqrt(e00), lax.rsqrt(f22)
                new = jnp.where(row_of > r + 3, new, old)
                new = jnp.where(row_of == r, r0 * root, new)
                new = jnp.where(row_of == r + 1, s1 * (root * lax.rsqrt(det)), new)
                new = jnp.where(row_of == r + 2, r2 * later, new)
                new = jnp.where(row_of == r + 3, s3 * (later * lax.rsqrt(second)), new)
            blocks[i] = new
    inverse = jnp.concatenate(blocks, axis=0)[:, rank:]
    ortho_ref[...] = lax.dot_general(
        left_ref[...], inverse, (((1,), (1,)), ((), ())), precision=HIGH,
        preferred_element_type=jnp.float32,
    )
    right = jnp.dot(
        inverse, total_ref[:, :cols], precision=HIGH, preferred_element_type=jnp.float32
    )
    right_ref[...] = right
    squares = lax.dot_general(
        jnp.ones((tile, cols), jnp.float32), right * right, (((1,), (1,)), ((), ())),
        precision=HIGH, preferred_element_type=jnp.float32,
    )
    squares = jnp.concatenate([squares, squares], axis=1)
    for i in range(squares_ref.shape[0]):
        squares_ref[i] = squares


def blend(pieces_ref, momentum_ref, right_ref, blended_ref, packed_ref):
    blended = momentum_ref[...]
    for i in range(pieces_ref.shape[0]):
        blended = blended + pieces_ref[i]
    blended_ref[...] = blended
    left = lax.dot_general(
        blended, right_ref[...], (((1,), (1,)), ((), ())), precision=HIGH,
        preferred_element_type=jnp.float32,
    )
    half = left.shape[0] // 2
    packed = jnp.concatenate([left[:half], left[half:]], axis=1)
    for i in range(packed_ref.shape[0]):
        packed_ref[i] = packed


def project(packed_ref, blended_ref, left_ref, value_ref):
    packed = packed_ref[0]
    for i in range(1, packed_ref.shape[0]):
        packed = packed + packed_ref[i]
    rank = left_ref.shape[1]
    left = jnp.concatenate([packed[:, :rank], packed[:, rank:]], axis=0)
    left_ref[...] = left
    both = jnp.concatenate([blended_ref[...], left, left], axis=1)
    value_ref[...] = lax.dot_general(
        left, both, (((0,), (0,)), ((), ())), precision=HIGH, preferred_element_type=jnp.float32
    )


def finish(ortho_ref, right_ref, squares_ref, blended_ref, momentum_ref, factor_ref, update_ref, *, scale):
    rank = ortho_ref.shape[1]
    squares = squares_ref[0]
    for i in range(1, squares_ref.shape[0]):
        squares = squares + squares_ref[i]
    root = jnp.sqrt(squares[:1, :rank] + 1e-06)
    row = lax.broadcasted_iota(jnp.int32, (rank, rank), 0)
    lane = lax.broadcasted_iota(jnp.int32, (rank, rank), 1)
    root = jnp.sum(jnp.where(row == lane, root, 0.0), axis=1, keepdims=True)
    right = right_ref[...]
    factor = right / root
    factor_ref[...] = factor
    ortho = ortho_ref[...]
    dot = functools.partial(jnp.dot, precision=HIGH, preferred_element_type=jnp.float32)
    momentum_ref[...] = blended_ref[...] - 0.05 * dot(ortho, right)
    update_ref[...] = (scale * dot(ortho, factor)).astype(update_ref.dtype)


def local_kernel(kernel, *out_shapes):
    return pl.pallas_call(
        kernel,
        out_shape=out_shapes,
        compiler_params=pltpu.CompilerParams(vmem_limit_bytes=4 * 1024 * 1024),
    )


def body(inputs, cotangent, momentum, right_prev):
    out_total = cotangent.shape[1]
    shards = lax.axis_size(SHARD)
    in_total = momentum.shape[1] * shards
    rank = right_prev.shape[1]
    rows, cols = momentum.shape
    f32 = functools.partial(jax.ShapeDtypeStruct, dtype=jnp.float32)
    pieces = gradient_rows(inputs, cotangent)
    blended, packed = local_kernel(
        blend, f32((rows, cols)), f32((shards, rows // 2, 2 * rank))
    )(pieces, momentum, right_prev.T)
    left_raw, value = local_kernel(
        project, f32((rows, rank)), f32((rank, cols + 2 * rank))
    )(exchanged(packed, SHARD), blended)
    ortho, right_rows, squares = local_kernel(
        eliminate, f32((rows, rank)), f32((rank, cols)), f32((shards, 8, 2 * rank))
    )(rep_total(value), left_raw)
    scale = (out_total * in_total / rank) ** 0.5
    new_momentum, factor_rows, update = local_kernel(
        functools.partial(finish, scale=scale),
        f32((rows, cols)), f32((rank, cols)), jax.ShapeDtypeStruct((rows, cols), jnp.bfloat16),
    )(ortho, right_rows, exchanged(squares, SHARD), blended)
    return (new_momentum, factor_rows.T, update)


def solution(mesh):
    finer = Mesh(mesh.devices.reshape(4, 12, 2, mesh.shape["shard"]), (*REP, SHARD))
    in_specs = (P(REP, SHARD), P(REP, None), P(REP, SHARD), P(SHARD, None))
    out_specs = (P(REP, SHARD), P(SHARD, None), P(REP, SHARD))
    return jax.shard_map(body, mesh=finer, in_specs=in_specs, out_specs=out_specs, check_vma=False)
```

```python
import functools

import jax
import jax.numpy as jnp
from jax import lax
from jax.experimental import pallas as pl
from jax.experimental.pallas import tpu as pltpu
from jax.sharding import Mesh
from jax.sharding import PartitionSpec as P

X, Z, CORE, SHARD = "rep_x", "rep_z", "rep_core", "shard"
REP = (X, Z, CORE)
CLASSES = 3
HIGH = lax.Precision.HIGHEST


def exchanged(pieces, axis, groups=None):
    return lax.all_to_all(pieces, axis, 0, 0, tiled=True, axis_index_groups=groups)


def from_everyone(value, axis):
    count = lax.axis_size(axis)
    return exchanged(jnp.broadcast_to(value[None], (count, *value.shape)), axis)


def sent(value, axis, distance):
    size = lax.axis_size(axis)
    return lax.ppermute(value, axis, [(i, (i + distance) % size) for i in range(size)])


def gated(value, *earlier):
    return lax.optimization_barrier((value, *earlier))[0]


def gradient_rows(inputs, cotangent):
    nx, nz = lax.axis_size(X), lax.axis_size(Z)
    na, nb = nz // CLASSES, CLASSES
    cols = inputs.shape[1]
    rows = cotangent.shape[1] // (nx * nz * 2)
    x, z, core = lax.axis_index(X), lax.axis_index(Z), lax.axis_index(CORE)
    half = na * nb * rows * 7 // 12 // 8 * 8

    partial = lax.dot_general(
        cotangent, inputs, (((0,), (0,)), ((), ())), preferred_element_type=jnp.float32
    ).reshape(nx, na, nb, 2, rows, cols)

    def piece(ahead, which, source=partial):
        at_x = lax.dynamic_index_in_dim(source, (x + ahead) % nx, 0, keepdims=False)
        return lax.dynamic_index_in_dim(at_x, which, 2, keepdims=False).reshape(-1, cols)

    near = jnp.stack([piece(ahead, 1 - core) for ahead in (1, 3, 0)])
    far, near, mine_far = lax.optimization_barrier((piece(2, 1 - core), near, piece(2, core)))
    far = sent(far, CORE, 1)
    near = sent(near, CORE, 1)
    far_up, far_down = mine_far[:half] + far[:half], mine_far[half:] + far[half:]
    relay_up = sent(far_up, X, 1)
    relay_down = sent(far_down, X, -1)
    near = gated(near, far_up, far_down)
    later = gated(partial, far_up, far_down)
    mine_before, mine_after, mine = (piece(ahead, core, later) for ahead in (1, 3, 0))
    before_low = mine_before[:half] + near[0, :half]
    before_high = mine_before[half:] + near[0, half:]
    after_low = mine_after[:half] + near[1, :half]
    after_high = mine_after[half:] + near[1, half:]
    high_below = sent(before_high, X, 1)
    low_above = sent(after_low, X, -1)
    relay_up = gated(relay_up, before_low, before_high, after_low)
    low_below = sent(before_low + relay_up, X, 1)
    relay_down = gated(relay_down, after_high, before_high, after_low)
    high_above = sent(after_high + relay_down, X, -1)
    own = lax.optimization_barrier(mine + near[2])
    low = own[:half] + low_below + low_above
    high = own[half:] + high_below + high_above
    over_x = jnp.concatenate([low, high], axis=0).reshape(na, nb, rows, cols)

    kind = z % nb

    def of_class(ahead):
        return lax.dynamic_index_in_dim(over_x, (kind + ahead) % nb, 1, keepdims=False)

    up = sent(of_class(1), Z, 1)
    down = sent(of_class(nb - 1), Z, -1)
    over_near_z = of_class(0) + up + down
    groups = [[a * nb + b for a in range(na)] for b in range(nb)]
    return exchanged(over_near_z, Z, groups)


def rep_total(value):
    members = lax.axis_size((X, CORE))
    piece = value.reshape(members, value.shape[0] // members, value.shape[1])
    piece = jnp.sum(exchanged(piece, (X, CORE)), axis=0)
    piece = jnp.sum(from_everyone(piece, Z), axis=0)
    return from_everyone(piece, (X, CORE)).reshape(value.shape)


def eliminate(total_ref, left_ref, ortho_ref, right_ref, squares_ref):
    rank = left_ref.shape[1]
    cols = right_ref.shape[1]
    tile = 8
    wide = 2 * rank
    full = total_ref[:, cols : cols + wide]
    row = lax.broadcasted_iota(jnp.int32, (rank, wide), 0)
    lane = lax.broadcasted_iota(jnp.int32, (rank, wide), 1)
    diagonal = jnp.where(lane == row, full, 0.0)
    down = lax.rsqrt(jnp.sum(diagonal, axis=1, keepdims=True))
    along = lax.rsqrt(jnp.sum(diagonal + jnp.where(lane == row + rank, 1.0, 0.0), axis=0, keepdims=True))
    scaled = jnp.where(lane < rank, full * down * along, jnp.where(lane == row + rank, down, 0.0))
    blocks = [scaled[b * tile : (b + 1) * tile, :] for b in range(rank // tile)]
    row_of = lax.broadcasted_iota(jnp.int32, (tile, wide), 0)
    full_tile = functools.partial(jnp.broadcast_to, shape=(tile, wide))
    for k in range(0, rank, 4):
        b, r = divmod(k, tile)
        r0, r1, r2, r3 = (full_tile(blocks[b][r + i : r + i + 1, :]) for i in range(4))

        def at(row, j, k=k):
            return full_tile(row[:, k + j : k + j + 1])

        e00, e01, e02, e03 = (at(r0, j) for j in range(4))
        e11, e12, e13 = (at(r1, j) for j in range(1, 4))
        e22, e23, e33 = at(r2, 2), at(r2, 3), at(r3, 3)
        det = e00 * e11 - e01 * e01
        inv = 1.0 / det
        s0, s1 = e11 * r0 - e01 * r1, e00 * r1 - e01 * r0
        u02, u03 = (e11 * e02 - e01 * e12) * inv, (e11 * e03 - e01 * e13) * inv
        u12, u13 = (e00 * e12 - e01 * e02) * inv, (e00 * e13 - e01 * e03) * inv
        f22 = e22 - e02 * u02 - e12 * u12
        f23 = e23 - e02 * u03 - e12 * u13
        f33 = e33 - e03 * u03 - e13 * u13
        t0, t1 = s0 * inv, s1 * inv
        r2, r3 = r2 - e02 * t0 - e12 * t1, r3 - e03 * t0 - e13 * t1
        second = f22 * f33 - f23 * f23
        inv = 1.0 / second
        s3 = f22 * r3 - f23 * r2
        t2, t3 = (f33 * r2 - f23 * r3) * inv, s3 * inv
        t0, t1 = t0 - u02 * t2 - u03 * t3, t1 - u12 * t2 - u13 * t3
        for i in range(b, rank // tile):
            old = blocks[i]
            new = (old - at(old, 0) * t0 - at(old, 1) * t1) - (at(old, 2) * t2 + at(old, 3) * t3)
            if i == b:
                root, later = lax.rsqrt(e00), lax.rsqrt(f22)
                new = jnp.where(row_of > r + 3, new, old)
                new = jnp.where(row_of == r, r0 * root, new)
                new = jnp.where(row_of == r + 1, s1 * (root * lax.rsqrt(det)), new)
                new = jnp.where(row_of == r + 2, r2 * later, new)
                new = jnp.where(row_of == r + 3, s3 * (later * lax.rsqrt(second)), new)
            blocks[i] = new
    inverse = jnp.concatenate(blocks, axis=0)[:, rank:]
    ortho_ref[...] = lax.dot_general(
        left_ref[...], inverse, (((1,), (1,)), ((), ())), precision=HIGH,
        preferred_element_type=jnp.float32,
    )
    right = jnp.dot(
        inverse, total_ref[:, :cols], precision=HIGH, preferred_element_type=jnp.float32
    )
    right_ref[...] = right
    squares = lax.dot_general(
        jnp.ones((tile, cols), jnp.float32), right * right, (((1,), (1,)), ((), ())),
        precision=HIGH, preferred_element_type=jnp.float32,
    )
    squares = jnp.concatenate([squares, squares], axis=1)
    for i in range(squares_ref.shape[0]):
        squares_ref[i] = squares


def blend(pieces_ref, momentum_ref, right_ref, blended_ref, packed_ref):
    blended = momentum_ref[...]
    for i in range(pieces_ref.shape[0]):
        blended = blended + pieces_ref[i]
    blended_ref[...] = blended
    left = lax.dot_general(
        blended, right_ref[...], (((1,), (1,)), ((), ())), precision=HIGH,
        preferred_element_type=jnp.float32,
    )
    half = left.shape[0] // 2
    packed = jnp.concatenate([left[:half], left[half:]], axis=1)
    for i in range(packed_ref.shape[0]):
        packed_ref[i] = packed


def project(packed_ref, blended_ref, left_ref, value_ref):
    packed = packed_ref[0]
    for i in range(1, packed_ref.shape[0]):
        packed = packed + packed_ref[i]
    rank = left_ref.shape[1]
    left = jnp.concatenate([packed[:, :rank], packed[:, rank:]], axis=0)
    left_ref[...] = left
    both = jnp.concatenate([blended_ref[...], left, left], axis=1)
    value_ref[...] = lax.dot_general(
        left, both, (((0,), (0,)), ((), ())), precision=HIGH, preferred_element_type=jnp.float32
    )


def finish(ortho_ref, right_ref, squares_ref, blended_ref, momentum_ref, factor_ref, update_ref, *, scale):
    rank = ortho_ref.shape[1]
    squares = squares_ref[0]
    for i in range(1, squares_ref.shape[0]):
        squares = squares + squares_ref[i]
    root = jnp.sqrt(squares[:1, :rank] + 1e-06)
    row = lax.broadcasted_iota(jnp.int32, (rank, rank), 0)
    lane = lax.broadcasted_iota(jnp.int32, (rank, rank), 1)
    root = jnp.sum(jnp.where(row == lane, root, 0.0), axis=1, keepdims=True)
    right = right_ref[...]
    factor = right / root
    factor_ref[...] = factor
    ortho = ortho_ref[...]
    dot = functools.partial(jnp.dot, precision=HIGH, preferred_element_type=jnp.float32)
    momentum_ref[...] = blended_ref[...] - 0.05 * dot(ortho, right)
    update_ref[...] = (scale * dot(ortho, factor)).astype(update_ref.dtype)


def local_kernel(kernel, *out_shapes):
    return pl.pallas_call(
        kernel,
        out_shape=out_shapes,
        compiler_params=pltpu.CompilerParams(vmem_limit_bytes=4 * 1024 * 1024),
    )


def body(inputs, cotangent, momentum, right_prev):
    out_total = cotangent.shape[1]
    shards = lax.axis_size(SHARD)
    in_total = momentum.shape[1] * shards
    rank = right_prev.shape[1]
    rows, cols = momentum.shape
    f32 = functools.partial(jax.ShapeDtypeStruct, dtype=jnp.float32)
    pieces = gradient_rows(inputs, cotangent)
    blended, packed = local_kernel(
        blend, f32((rows, cols)), f32((shards, rows // 2, 2 * rank))
    )(pieces, momentum, right_prev.T)
    left_raw, value = local_kernel(
        project, f32((rows, rank)), f32((rank, cols + 2 * rank))
    )(exchanged(packed, SHARD), blended)
    ortho, right_rows, squares = local_kernel(
        eliminate, f32((rows, rank)), f32((rank, cols)), f32((shards, 8, 2 * rank))
    )(rep_total(value), left_raw)
    scale = (out_total * in_total / rank) ** 0.5
    new_momentum, factor_rows, update = local_kernel(
        functools.partial(finish, scale=scale),
        f32((rows, cols)), f32((rank, cols)), jax.ShapeDtypeStruct((rows, cols), jnp.bfloat16),
    )(ortho, right_rows, exchanged(squares, SHARD), blended)
    return (new_momentum, factor_rows.T, update)


def solution(mesh):
    finer = Mesh(mesh.devices.reshape(4, 12, 2, mesh.shape["shard"]), (*REP, SHARD))
    in_specs = (P(REP, SHARD), P(REP, None), P(REP, SHARD), P(SHARD, None))
    out_specs = (P(REP, SHARD), P(SHARD, None), P(REP, SHARD))
    return jax.shard_map(body, mesh=finer, in_specs=in_specs, out_specs=out_specs, check_vma=False)
```
